128 devices in a mesh: data: 1, sp: 128 (over z, y, x, core).
Axes of the slice: x: 4, y: 4, z: 4, core: 2. Of those that a mesh axis runs over, the one named last changes fastest.
Arguments:
- latent: bfloat16 [1, 768, 1024, 384], P('data', 'sp')
- ln_gain: bfloat16 [4, 384], replicated
- ln_bias: bfloat16 [4, 384], replicated
- w_qkv: bfloat16 [2, 384, 3, 6, 64], replicated
- w_out: bfloat16 [2, 6, 64, 384], replicated
- w_up: bfloat16 [2, 384, 1536], replicated
- w_down: bfloat16 [2, 1536, 384], replicated
Outputs:
- output: bfloat16 [1, 768, 1024, 384], P('data', 'sp')
All inputs are finite; a program needn't handle non-finite values.
Results may differ from the reference program's by a relative error of at most 0.0106958.
Values are sent between devices in bfloat16 or wider.
A program may use at most 1 GiB of HBM per device.

```python
import jax
import jax.numpy as jnp
from jax import lax
from functools import partial

FRAMES = 768
PATCHES = 1024
WIDTH = 384
NUM_HEADS = 6
HEAD_DIM = WIDTH // NUM_HEADS
LN_EPS = 1e-6


def setup_inputs(seed: int = 0, part: int = 0) -> dict:
    part_key = jax.random.fold_in(jax.random.key(seed), part)
    noise_key, frame_key, patch_key = jax.random.split(part_key, 3)
    noise = jax.random.normal(noise_key, (1, FRAMES, PATCHES, WIDTH), jnp.float32)
    frame_sig = jax.random.normal(frame_key, (1, FRAMES, 1, WIDTH), jnp.float32)
    patch_sig = jax.random.normal(patch_key, (1, 1, PATCHES, WIDTH), jnp.float32)
    latent = 0.6 * noise + frame_sig + 0.8 * patch_sig
    weight_keys = jax.random.split(jax.random.key(seed + 1), 6)
    qk_boost = jnp.array([1.3, 1.3, 1.0], jnp.float32).reshape(1, 1, 3, 1, 1)
    ln_gain = 1.0 + 0.4 * jax.random.normal(weight_keys[0], (4, WIDTH), jnp.float32)
    ln_bias = 0.5 * jax.random.normal(weight_keys[1], (4, WIDTH), jnp.float32)
    w_qkv = jax.random.normal(weight_keys[2], (2, WIDTH, 3, NUM_HEADS, HEAD_DIM), jnp.float32) * qk_boost * WIDTH ** -0.5
    w_out = jax.random.normal(weight_keys[3], (2, NUM_HEADS, HEAD_DIM, WIDTH), jnp.float32) * WIDTH ** -0.5
    w_up = jax.random.normal(weight_keys[4], (2, WIDTH, 4 * WIDTH), jnp.float32) * WIDTH ** -0.5
    w_down = jax.random.normal(weight_keys[5], (2, 4 * WIDTH, WIDTH), jnp.float32) * (4 * WIDTH) ** -0.5
    return {
        'latent': latent.astype(jnp.bfloat16),
        'ln_gain': ln_gain.astype(jnp.bfloat16),
        'ln_bias': ln_bias.astype(jnp.bfloat16),
        'w_qkv': w_qkv.astype(jnp.bfloat16),
        'w_out': w_out.astype(jnp.bfloat16),
        'w_up': w_up.astype(jnp.bfloat16),
        'w_down': w_down.astype(jnp.bfloat16),
    }


def layer_norm(tokens, gain_vec, shift_vec):
    as_float = tokens.astype(jnp.float32)
    mean_val = jnp.mean(as_float, axis=-1, keepdims=True)
    centered = as_float - mean_val
    variance = jnp.mean(centered * centered, axis=-1, keepdims=True)
    normed = centered * lax.rsqrt(variance + LN_EPS) * gain_vec.astype(jnp.float32) + shift_vec.astype(jnp.float32)
    return normed.astype(jnp.bfloat16)


def seq_block(sequence, layer_idx, ln_gain, ln_bias, w_qkv, w_out, w_up, w_down):
    length = sequence.shape[0]
    normed = layer_norm(sequence, ln_gain[2 * layer_idx], ln_bias[2 * layer_idx])
    qkv_all = jnp.dot(normed, w_qkv[layer_idx].reshape(WIDTH, 3 * WIDTH), preferred_element_type=jnp.float32).astype(jnp.bfloat16)
    qkv_all = qkv_all.reshape(length, 3, NUM_HEADS, HEAD_DIM).astype(jnp.float32)
    scores = jnp.einsum('qhk,phk->hqp', qkv_all[:, 0], qkv_all[:, 1]) * HEAD_DIM ** -0.5
    attn_probs = jax.nn.softmax(scores, axis=-1).astype(jnp.bfloat16)
    attended = jnp.einsum('hqp,phk->qhk', attn_probs.astype(jnp.float32), qkv_all[:, 2]).astype(jnp.bfloat16)
    projected = jnp.dot(attended.reshape(length, WIDTH), w_out[layer_idx].reshape(WIDTH, WIDTH), preferred_element_type=jnp.float32)
    residual = (sequence.astype(jnp.float32) + projected).astype(jnp.bfloat16)
    normed_mlp = layer_norm(residual, ln_gain[2 * layer_idx + 1], ln_bias[2 * layer_idx + 1])
    hidden = jax.nn.gelu(jnp.dot(normed_mlp, w_up[layer_idx], preferred_element_type=jnp.float32), approximate=True).astype(jnp.bfloat16)
    result = residual.astype(jnp.float32) + jnp.dot(hidden, w_down[layer_idx], preferred_element_type=jnp.float32)
    return result.astype(jnp.bfloat16)


def reference(latent, ln_gain, ln_bias, w_qkv, w_out, w_up, w_down):
    space_fn = partial(seq_block, layer_idx=0, ln_gain=ln_gain, ln_bias=ln_bias, w_qkv=w_qkv, w_out=w_out, w_up=w_up, w_down=w_down)
    spatial = lax.map(space_fn, latent[0])
    time_fn = partial(seq_block, layer_idx=1, ln_gain=ln_gain, ln_bias=ln_bias, w_qkv=w_qkv, w_out=w_out, w_up=w_up, w_down=w_down)
    temporal = lax.map(time_fn, jnp.swapaxes(spatial, 0, 1))
    return jnp.swapaxes(temporal, 0, 1)[None]
```

```python
import functools
import jax
import jax.numpy as jnp
from jax import lax
from jax.experimental import pallas as pl
from jax.experimental.pallas import tpu as pltpu
from jax.sharding import PartitionSpec as P

LN_EPS = 1e-6
HEADS = 6
HEAD_DIM = 64
BF = jnp.bfloat16
F32 = jnp.float32
SUBL = 8
TILE = 128
CHUNK = 256
EXP2_SCALE = 1.4426950408889634 * HEAD_DIM ** -0.5


def layer_norm(xf, gain, shift):
    mean = jnp.mean(xf, axis=-1, keepdims=True)
    cen = xf - mean
    var = jnp.mean(cen * cen, axis=-1, keepdims=True)
    return (cen * lax.rsqrt(var + LN_EPS) * gain + shift).astype(BF)


def dot(a, b):
    return jnp.dot(a, b, preferred_element_type=F32)


def dot_t(a, b):
    return lax.dot_general(a, b, (((1,), (1,)), ((), ())), preferred_element_type=F32)


def gelu(x):
    inner = x * (0.7978845608028654 + 0.035677408136300125 * (x * x))
    half = 0.5 * x
    return half + half * jnp.tanh(inner)


def attend(q, k_at, v_at):
    lane = lax.broadcasted_iota(jnp.int32, (TILE, 128), 1)
    outs = []
    for pair in range(HEADS // 2):
        qp = q[:, 128 * pair:128 * pair + 128]
        zero = jnp.zeros_like(qp)
        qm = jnp.concatenate([jnp.where(lane < HEAD_DIM, qp, zero), jnp.where(lane < HEAD_DIM, zero, qp)], axis=0)
        s = dot_t(k_at(pair), qm)
        top = jnp.max(s, axis=0, keepdims=True)
        e = jnp.exp2((s - top) * EXP2_SCALE)
        total = jnp.sum(e, axis=0, keepdims=True)
        o = dot(v_at(pair), e.astype(BF)) * (1.0 / total)
        o = jnp.concatenate([o[:HEAD_DIM, :TILE], o[HEAD_DIM:, TILE:]], axis=0)
        outs.append(o.T.astype(BF))
    return jnp.concatenate(outs, axis=1)


def finish(xb, o, gain, shift, wout, wup, wdown):
    h = (xb.astype(F32) + dot(o, wout)).astype(BF)
    hf = h.astype(F32)
    a = layer_norm(hf, gain, shift)
    u = gelu(dot(a, wup)).astype(BF)
    return hf + dot(u, wdown)


def kernel(ndev, frames, x_ref, gain_ref, shift_ref, wqk_ref, wv_ref, wout_ref, wup_ref, wdown_ref, out_ref,
           wvt, qs, ks, vts, os_, sendbuf, recv, xt, q1, k1, v1t, y1, send_sem, recv_sem, loc_sem):
    patches = ndev * SUBL
    width = HEADS * HEAD_DIM
    seq = frames * ndev
    me = lax.axis_index('sp')
    core, cx, cy, cz = me % 2, (me // 2) % 4, (me // 8) % 4, me // 32
    nchunk = patches // CHUNK

    for l in range(2):
        wvt[l] = wv_ref[l].astype(F32).T.astype(BF)

    def peer(i):
        i = (i * 37) % ndev
        dc, dx, dy, dz = i % 2, (i // 2) % 4, (i // 8) % 4, i // 32
        return ((cz + dz) % 4) * 32 + ((cy + dy) % 4) * 8 + ((cx + dx) % 4) * 2 + (core + dc) % 2

    def send_round(stage, dst, j):
        src = sendbuf.at[stage, j]
        own = pltpu.make_async_copy(src.at[me], dst.at[j, me], loc_sem.at[stage, j])
        own.start()

        def body(i, c):
            to = peer(i)
            pltpu.make_async_remote_copy(
                src_ref=src.at[to], dst_ref=dst.at[j, me],
                send_sem=send_sem.at[stage, j], recv_sem=recv_sem.at[stage, j],
                device_id={'sp': to}, device_id_type=pl.DeviceIdType.MESH).start()
            return c
        lax.fori_loop(1, ndev, body, 0)

    def wait_bytes(ref, sem):
        pltpu.make_async_copy(ref, ref, sem).wait()

    def wait_arrived(stage, dst, j):
        pltpu.make_async_copy(sendbuf.at[stage, j, 0], dst.at[j, 0], loc_sem.at[stage, j]).wait()
        wait_bytes(dst.at[j, pl.ds(0, ndev - 1)], recv_sem.at[stage, j])

    def wait_sent(stage, j):
        wait_bytes(sendbuf.at[stage, j, pl.ds(0, ndev - 1)], send_sem.at[stage, j])

    def params(l):
        g = gain_ref[...].astype(F32)
        b = shift_ref[...].astype(F32)
        return g[2 * l:2 * l + 1], b[2 * l:2 * l + 1], g[2 * l + 1:2 * l + 2], b[2 * l + 1:2 * l + 2]

    ga, ba, gm, bm = params(0)

    def frame_step(j, carry):
        def qkv_step(c, cc):
            rows = pl.ds(pl.multiple_of(c * CHUNK, CHUNK), CHUNK)
            a = layer_norm(x_ref[j, rows, :].astype(F32), ga, ba)
            qk = dot(a, wqk_ref[0]).astype(BF)
            qs[rows, :] = qk[:, :width]
            ks[rows, :] = qk[:, width:]
            vts[:, rows] = dot_t(wvt[0], a).astype(BF)
            return cc
        lax.fori_loop(0, nchunk, qkv_step, 0)

        def tile_step(t, cc):
            rows = pl.ds(pl.multiple_of(t * TILE, TILE), TILE)
            os_[rows, :] = attend(qs[rows, :], lambda p: ks[:, 128 * p:128 * p + 128], lambda p: vts[128 * p:128 * p + 128, :])
            return cc
        lax.fori_loop(0, patches // TILE, tile_step, 0)

        def mlp_step(c, cc):
            rows = pl.ds(pl.multiple_of(c * CHUNK, CHUNK), CHUNK)
            y = finish(x_ref[j, rows, :], os_[rows, :], gm, bm, wout_ref[0], wup_ref[0], wdown_ref[0])
            dests = CHUNK // SUBL
            sendbuf[0, j, pl.ds(pl.multiple_of(c * dests, dests), dests)] = y.reshape(dests, SUBL, width).astype(BF)
            return cc
        lax.fori_loop(0, nchunk, mlp_step, 0)
        send_round(0, recv, j)
        return carry
    lax.fori_loop(0, frames, frame_step, 0)

    ga, ba, gm, bm = params(1)
    r_io = lax.broadcasted_iota(jnp.int32, (128, 128), 0)
    c_io = lax.broadcasted_iota(jnp.int32, (128, 128), 1)
    to_seq = jnp.where((r_io // 16 == c_io % 8) & (r_io % 16 == c_io // 8), 1.0, 0.0).astype(BF)
    to_tok = jnp.where((r_io % 8 == c_io // 16) & (r_io // 8 == c_io % 16), 1.0, 0.0).astype(BF)

    def kv_step(j, carry):
        wait_arrived(0, recv, j)

        def perm_step(g, cc):
            blk = recv[j, pl.ds(g * 16, 16)].astype(F32).reshape(128, width).astype(BF)
            seqd = dot(to_seq, blk).astype(BF)
            for p in range(SUBL):
                xt[j, p, pl.ds(pl.multiple_of(g * 16, 16), 16), :] = seqd[16 * p:16 * p + 16]
            return cc
        lax.fori_loop(0, ndev // 16, perm_step, 0)

        def qkv_step(c, cc):
            xb = xt[j, pl.ds(2 * c, 2)].reshape(2 * ndev, width)
            a = layer_norm(xb.astype(F32), ga, ba)
            qk = dot(a, wqk_ref[1]).astype(BF)
            vt = dot_t(wvt[1], a).astype(BF)
            cols = pl.ds(pl.multiple_of(j * ndev, ndev), ndev)
            for i in range(2):
                part = slice(i * ndev, (i + 1) * ndev)
                q1[2 * c + i, cols, :] = qk[part, :width]
                k1[2 * c + i, cols, :] = qk[part, width:]
                v1t[2 * c + i, :, cols] = vt[:, part]
            return cc
        lax.fori_loop(0, SUBL // 2, qkv_step, 0)
        return carry
    lax.fori_loop(0, frames, kv_step, 0)

    def time_step(j, carry):
        cols = pl.ds(pl.multiple_of(j * ndev, ndev), ndev)

        def tile_step(p, cc):
            rows = pl.ds(pl.multiple_of(p * TILE, TILE), TILE)
            os_[rows, :] = attend(q1[p, cols, :], lambda h: k1[p, :, 128 * h:128 * h + 128], lambda h: v1t[p, 128 * h:128 * h + 128, :])
            return cc
        lax.fori_loop(0, SUBL, tile_step, 0)

        def mlp_step(c, cc):
            rows = pl.ds(pl.multiple_of(c * CHUNK, CHUNK), CHUNK)
            y = finish(xt[j, pl.ds(2 * c, 2)].reshape(CHUNK, width), os_[rows, :], gm, bm, wout_ref[1], wup_ref[1], wdown_ref[1])
            y1[pl.ds(2 * c, 2)] = y.astype(BF).reshape(2, ndev, width)
            return cc
        lax.fori_loop(0, SUBL // 2, mlp_step, 0)

        def perm_step(g, cc):
            blk = y1[:, pl.ds(pl.multiple_of(g * 16, 16), 16), :].reshape(128, width)
            tok = dot(to_tok, blk)
            sendbuf[1, j, pl.ds(g * 16, 16)] = tok.reshape(16, SUBL, width).astype(BF)
            return cc
        lax.fori_loop(0, ndev // 16, perm_step, 0)
        send_round(1, out_ref, j)
        return carry
    lax.fori_loop(0, frames, time_step, 0)

    def drain(j, carry):
        wait_sent(0, j)
        wait_sent(1, j)
        wait_arrived(1, out_ref, j)
        return carry
    lax.fori_loop(0, frames, drain, 0)


def solution(mesh):
    ndev = mesh.shape['sp']
    act_spec = P('data', 'sp', None, None)

    def local_run(latent, ln_gain, ln_bias, w_qkv, w_out, w_up, w_down):
        _, frames, patches, width = latent.shape
        wqkv = w_qkv.reshape(2, width, 3 * width)
        wqk, wv = wqkv[:, :, :2 * width], wqkv[:, :, 2 * width:]
        seq = frames * ndev
        out = pl.pallas_call(
            functools.partial(kernel, ndev, frames),
            out_shape=jax.ShapeDtypeStruct((frames, ndev, SUBL, width), BF),
            in_specs=[pl.BlockSpec(memory_space=pltpu.VMEM)] * 8,
            out_specs=pl.BlockSpec(memory_space=pl.ANY),
            scratch_shapes=[
                pltpu.VMEM((2, width, width), BF),
                pltpu.VMEM((patches, width), BF),
                pltpu.VMEM((patches, width), BF),
                pltpu.VMEM((width, patches), BF),
                pltpu.VMEM((patches, width), BF),
                pltpu.VMEM((2, frames, ndev, SUBL, width), BF),
                pltpu.VMEM((frames, ndev, SUBL, width), BF),
                pltpu.VMEM((frames, SUBL, ndev, width), BF),
                pltpu.VMEM((SUBL, seq, width), BF),
                pltpu.VMEM((SUBL, seq, width), BF),
                pltpu.VMEM((SUBL, width, seq), BF),
                pltpu.VMEM((SUBL, ndev, width), BF),
                pltpu.SemaphoreType.DMA((2, frames)),
                pltpu.SemaphoreType.DMA((2, frames)),
                pltpu.SemaphoreType.DMA((2, frames)),
            ],
            compiler_params=pltpu.CompilerParams(has_side_effects=True, vmem_limit_bytes=67043328),
            name='latte_blocks',
        )(latent[0], ln_gain, ln_bias, wqk, wv, w_out.reshape(2, width, width), w_up, w_down)
        return out.reshape(1, frames, patches, width)

    return jax.shard_map(local_run, mesh=mesh, in_specs=(act_spec, P(), P(), P(), P(), P(), P()), out_specs=act_spec, check_vma=False)
```

```python
import functools
import jax
import jax.numpy as jnp
from jax import lax
from jax.experimental import pallas as pl
from jax.experimental.pallas import tpu as pltpu
from jax.sharding import PartitionSpec as P

LN_EPS = 1e-6
HEADS = 6
HEAD_DIM = 64
BF = jnp.bfloat16
F32 = jnp.float32
SUBL = 8
TILE = 256
PLANES = 4
ORDER = (2, 6, 4, 3, 7, 5, 1)
KEYS = 256
GROUP = 8
CHUNK = 256
HIDDEN = 768
MLPS = 2
EXP2_SCALE = 1.4426950408889634 * HEAD_DIM ** -0.5


def layer_norm(xf, gain, shift):
    mean = jnp.mean(xf, axis=-1, keepdims=True)
    cen = xf - mean
    var = jnp.mean(cen * cen, axis=-1, keepdims=True)
    return (cen * lax.rsqrt(var + LN_EPS) * gain + shift).astype(BF)


def dot(a, b):
    return jnp.dot(a, b, preferred_element_type=F32)


def dot_t(a, b):
    return lax.dot_general(a, b, (((1,), (1,)), ((), ())), preferred_element_type=F32)


def gelu(x):
    inner = x * (0.7978845608028654 + 0.035677408136300125 * (x * x))
    half = 0.5 * x
    return half + half * jnp.tanh(inner)


def score(q, k_at, keys, head, s_ref, m_ref):
    lane = lax.broadcasted_iota(jnp.int32, (TILE, 128), 1)
    qm = jnp.where(lax.div(lane, HEAD_DIM) == head % 2, q, jnp.zeros_like(q))
    slot = head % 2
    top = None
    for c in range(keys // KEYS):
        s = dot_t(k_at(c), qm)
        s_ref[slot, c * KEYS:(c + 1) * KEYS, :] = s
        t = jnp.max(s.reshape(KEYS // GROUP, GROUP, TILE), axis=0)
        top = t if top is None else jnp.maximum(top, t)
        yield
    m_ref[slot] = jnp.broadcast_to(jnp.max(top, axis=0, keepdims=True), (8, TILE))
    yield


def mix(v_at, keys, head, s_ref, m_ref, out):
    slot = head % 2
    top = m_ref[slot, 0:1, :]
    total = None
    o = None
    for c in range(keys // KEYS):
        e = jnp.exp2((s_ref[slot, c * KEYS:(c + 1) * KEYS, :] - top) * EXP2_SCALE)
        t = jnp.sum(e.reshape(KEYS // GROUP, GROUP, TILE), axis=0)
        total = t if total is None else total + t
        d = dot(v_at(c), e.astype(BF))
        o = d if o is None else o + d
        yield
    out.append(o * (1.0 / jnp.sum(total, axis=0, keepdims=True)))
    yield


def together(*steps):
    live = list(steps)
    while live:
        live = [g for g in live if next(g, live) is not live]


def attention(tiles, q_at, k_at, v_at, keys, s_ref, m_ref, put):
    def scores(t, head):
        return score(q_at(t, head // 2), lambda c: k_at(t, head // 2, c), keys, head, s_ref, m_ref)

    together(scores(0, 0))

    def step(t, carry):
        after = lax.rem(t + 1, tiles)
        out = []
        for head in range(HEADS):
            ahead = scores(t, head + 1) if head + 1 < HEADS else scores(after, 0)
            together(ahead, mix(lambda c: v_at(t, head, c), keys, head, s_ref, m_ref, out))
            if head % 2:
                put(t, head // 2, jnp.concatenate(out, axis=0).T.astype(BF))
                out = []
        return carry
    lax.fori_loop(0, tiles, step, 0)


def finish(xb, o, gain, shift, wout, wup, wdown, out):
    h = (xb.astype(F32) + dot(o, wout[...])).astype(BF)
    hf = h.astype(F32)
    yield
    a = layer_norm(hf, gain, shift)
    yield
    y = hf
    hidden = wup.shape[1]
    for c in range(0, hidden, HIDDEN):
        u = gelu(dot(a, wup[:, c:c + HIDDEN])).astype(BF)
        y = y + dot(u, wdown[c:c + HIDDEN, :])
        yield
    out.append(y)
    yield


def kernel(ndev, frames, x_ref, gain_ref, shift_ref, wqkv_ref, wout_ref, wup_ref, wdown_ref, out_ref,
           wqk, qs, ks, vts, os_, sendbuf, recv, xt, q1, k1, v1t, o1, y1, s_scr, m_scr, send_sem, recv_sem, loc_sem):
    patches = ndev * SUBL
    width = HEADS * HEAD_DIM
    seq = frames * ndev
    me = lax.axis_index('sp')
    core, cx = lax.rem(me, 2), lax.rem(lax.div(me, 2), 4)
    cy, cz = lax.rem(lax.div(me, 8), 4), lax.div(me, 32)
    at_x = [lax.rem(cx + d, 4) * 2 for d in range(4)]
    at_core = [lax.rem(core + d, 2) for d in range(2)]
    nchunk = patches // CHUNK

    for l in range(2):
        wqk[l] = wqkv_ref[l, :2 * width, :].astype(F32).T.astype(BF)

    def send_to(stage, dst, j, to):
        pltpu.make_async_remote_copy(
            src_ref=sendbuf.at[stage, j, to], dst_ref=dst.at[j, me],
            send_sem=send_sem.at[stage, j], recv_sem=recv_sem.at[stage, j],
            device_id={'sp': to}, device_id_type=pl.DeviceIdType.MESH).start()

    def plane(g):
        return lax.rem(cz + lax.div(g, 4), 4) * 32 + lax.rem(cy + lax.rem(g, 4), 4) * 8

    def send_round(stage, dst, j):
        pltpu.make_async_copy(sendbuf.at[stage, j, me], dst.at[j, me], loc_sem.at[stage, j]).start()

        def column(g, c):
            send_to(stage, dst, j, plane(g) + at_x[0] + at_core[0])
            return c
        lax.fori_loop(1, ndev // 8, column, 0)

        def planes(i, c):
            for g in range(PLANES):
                base = plane(i * PLANES + g)
                for d in ORDER:
                    send_to(stage, dst, j, base + at_x[d // 2] + at_core[d % 2])
            return c
        lax.fori_loop(0, ndev // 8 // PLANES, planes, 0)

    def wait_bytes(ref, sem):
        pltpu.make_async_copy(ref, ref, sem).wait()

    def wait_arrived(stage, dst, j):
        pltpu.make_async_copy(sendbuf.at[stage, j, 0], dst.at[j, 0], loc_sem.at[stage, j]).wait()
        wait_bytes(dst.at[j, pl.ds(0, ndev - 1)], recv_sem.at[stage, j])

    def wait_sent(stage, j):
        wait_bytes(sendbuf.at[stage, j, pl.ds(0, ndev - 1)], send_sem.at[stage, j])

    def params(l):
        g = gain_ref[...].astype(F32)
        b = shift_ref[...].astype(F32)
        return g[2 * l:2 * l + 1], b[2 * l:2 * l + 1], g[2 * l + 1:2 * l + 2], b[2 * l + 1:2 * l + 2]

    ga, ba, gm, bm = params(0)

    def frame_step(j, carry):
        def qkv_step(c, cc):
            rows = pl.ds(pl.multiple_of(c * CHUNK, CHUNK), CHUNK)
            a = layer_norm(x_ref[j, rows, :].astype(F32), ga, ba)
            qk = dot(a, wqk[0]).astype(BF)
            qs[rows, :] = qk[:, :width]
            ks[rows, :] = qk[:, width:]
            vts[:, rows] = dot_t(wqkv_ref[0, 2 * width:, :], a).astype(BF)
            return cc
        lax.fori_loop(0, nchunk, qkv_step, 0)

        def put(t, pair, o):
            os_[pl.ds(pl.multiple_of(t * TILE, TILE), TILE), 128 * pair:128 * pair + 128] = o
        attention(
            patches // TILE,
            lambda t, p: qs[pl.ds(pl.multiple_of(t * TILE, TILE), TILE), 128 * p:128 * p + 128],
            lambda t, p, c: ks[c * KEYS:(c + 1) * KEYS, 128 * p:128 * p + 128],
            lambda t, h, c: vts[HEAD_DIM * h:HEAD_DIM * h + HEAD_DIM, c * KEYS:(c + 1) * KEYS],
            patches, s_scr, m_scr, put)

        def mlp_step(c, cc):
            outs = [[] for _ in range(MLPS)]
            rows = [pl.ds(pl.multiple_of((c * MLPS + i) * CHUNK, CHUNK), CHUNK) for i in range(MLPS)]
            together(*[finish(x_ref[j, r, :], os_[r, :], gm, bm, wout_ref.at[0], wup_ref.at[0], wdown_ref.at[0], out)
                       for r, out in zip(rows, outs)])
            dests = CHUNK // SUBL
            for i in range(MLPS):
                to = pl.ds(pl.multiple_of((c * MLPS + i) * dests, dests), dests)
                sendbuf[0, j, to] = outs[i][0].reshape(dests, SUBL, width).astype(BF)
            return cc
        lax.fori_loop(0, nchunk // MLPS, mlp_step, 0)
        send_round(0, recv, j)
        return carry

    lax.fori_loop(0, frames, frame_step, 0)

    ga, ba, gm, bm = params(1)
    r_io = lax.broadcasted_iota(jnp.int32, (128, 128), 0)
    c_io = lax.broadcasted_iota(jnp.int32, (128, 128), 1)
    to_seq = jnp.where((r_io // 16 == c_io % 8) & (r_io % 16 == c_io // 8), 1.0, 0.0).astype(BF)
    to_tok = jnp.where((r_io % 8 == c_io // 16) & (r_io // 8 == c_io % 16), 1.0, 0.0).astype(BF)

    def kv_step(j, carry):
        wait_arrived(0, recv, j)

        def perm_step(g, cc):
            blk = recv[j, pl.ds(g * 16, 16)].astype(F32).reshape(128, width).astype(BF)
            seqd = dot(to_seq, blk).astype(BF)
            for p in range(SUBL):
                xt[j, p, pl.ds(pl.multiple_of(g * 16, 16), 16), :] = seqd[16 * p:16 * p + 16]
            return cc
        lax.fori_loop(0, ndev // 16, perm_step, 0)

        def qkv_step(c, cc):
            xb = xt[j, pl.ds(2 * c, 2)].reshape(2 * ndev, width)
            a = layer_norm(xb.astype(F32), ga, ba)
            qk = dot(a, wqk[1]).astype(BF)
            vt = dot_t(wqkv_ref[1, 2 * width:, :], a).astype(BF)
            cols = pl.ds(pl.multiple_of(j * ndev, ndev), ndev)
            for i in range(2):
                part = slice(i * ndev, (i + 1) * ndev)
                q1[2 * c + i, cols, :] = qk[part, :width]
                k1[2 * c + i, cols, :] = qk[part, width:]
                v1t[2 * c + i, :, cols] = vt[:, part]
            return cc
        lax.fori_loop(0, SUBL // 2, qkv_step, 0)
        return carry
    lax.fori_loop(0, frames, kv_step, 0)

    def time_step(jj, carry):
        first = pl.multiple_of(jj * TILE, TILE)

        def put(p, pair, o):
            o1[p, :, 128 * pair:128 * pair + 128] = o
        attention(
            SUBL,
            lambda t, p: q1[t, pl.ds(first, TILE), 128 * p:128 * p + 128],
            lambda t, p, c: k1[t, c * KEYS:(c + 1) * KEYS, 128 * p:128 * p + 128],
            lambda t, h, c: v1t[t, HEAD_DIM * h:HEAD_DIM * h + HEAD_DIM, c * KEYS:(c + 1) * KEYS],
            seq, s_scr, m_scr, put)

        def half_step(half, carry):
            j = jj * (TILE // ndev) + half
            part = pl.ds(pl.multiple_of(half * ndev, ndev), ndev)

            def mlp_step(c, cc):
                outs = [[] for _ in range(MLPS)]
                at = [pl.ds((c * MLPS + i) * 2, 2) for i in range(MLPS)]
                together(*[finish(xt[j, r].reshape(CHUNK, width), o1[r, part, :].reshape(CHUNK, width), gm, bm,
                                  wout_ref.at[1], wup_ref.at[1], wdown_ref.at[1], out) for r, out in zip(at, outs)])
                for i in range(MLPS):
                    y1[at[i]] = outs[i][0].astype(BF).reshape(2, ndev, width)
                return cc
            lax.fori_loop(0, SUBL // 2 // MLPS, mlp_step, 0)

            def perm_step(g, cc):
                blk = y1[:, pl.ds(pl.multiple_of(g * 16, 16), 16), :].reshape(128, width)
                tok = dot(to_tok, blk)
                sendbuf[1, j, pl.ds(g * 16, 16)] = tok.reshape(16, SUBL, width).astype(BF)
                return cc
            lax.fori_loop(0, ndev // 16, perm_step, 0)
            send_round(1, out_ref, j)
            return carry
        lax.fori_loop(0, TILE // ndev, half_step, 0)
        return carry

    lax.fori_loop(0, seq // TILE, time_step, 0)

    def drain(j, carry):
        wait_sent(0, j)
        wait_sent(1, j)
        wait_arrived(1, out_ref, j)
        return carry
    lax.fori_loop(0, frames, drain, 0)


def solution(mesh):
    ndev = mesh.shape['sp']
    act_spec = P('data', 'sp', None, None)

    def local_run(latent, ln_gain, ln_bias, w_qkv, w_out, w_up, w_down):
        _, frames, patches, width = latent.shape
        wqkv_t = w_qkv.transpose(0, 2, 3, 4, 1).reshape(2, 3 * width, width)
        seq = frames * ndev
        out = pl.pallas_call(
            functools.partial(kernel, ndev, frames),
            out_shape=jax.ShapeDtypeStruct((frames, ndev, SUBL, width), BF),
            in_specs=[pl.BlockSpec(memory_space=pltpu.VMEM)] * 7,
            out_specs=pl.BlockSpec(memory_space=pl.ANY),
            scratch_shapes=[
                pltpu.VMEM((2, width, 2 * width), BF),
                pltpu.VMEM((patches, width), BF),
                pltpu.VMEM((patches, width), BF),
                pltpu.VMEM((width, patches), BF),
                pltpu.VMEM((patches, width), BF),
                pltpu.VMEM((2, frames, ndev, SUBL, width), BF),
                pltpu.VMEM((frames, ndev, SUBL, width), BF),
                pltpu.VMEM((frames, SUBL, ndev, width), BF),
                pltpu.VMEM((SUBL, seq, width), BF),
                pltpu.VMEM((SUBL, seq, width), BF),
                pltpu.VMEM((SUBL, width, seq), BF),
                pltpu.VMEM((SUBL, 2 * ndev, width), BF),
                pltpu.VMEM((SUBL, ndev, width), BF),
                pltpu.VMEM((2, max(patches, seq), TILE), F32),
                pltpu.VMEM((2, 8, TILE), F32),
                pltpu.SemaphoreType.DMA((2, frames)),
                pltpu.SemaphoreType.DMA((2, frames)),
                pltpu.SemaphoreType.DMA((2, frames)),
            ],
            compiler_params=pltpu.CompilerParams(has_side_effects=True, vmem_limit_bytes=67043328),
            name='latte_blocks',
        )(latent[0], ln_gain, ln_bias, wqkv_t, w_out.reshape(2, width, width), w_up, w_down)
        return out.reshape(1, frames, patches, width)

    return jax.shard_map(local_run, mesh=mesh, in_specs=(act_spec, P(), P(), P(), P(), P(), P()), out_specs=act_spec, check_vma=False)
```

```python
import functools
import jax
import jax.numpy as jnp
from jax import lax
from jax.experimental import pallas as pl
from jax.experimental.pallas import tpu as pltpu
from jax.sharding import PartitionSpec as P

LN_EPS = 1e-6
HEADS = 6
HEAD_DIM = 64
BF = jnp.bfloat16
F32 = jnp.float32
SUBL = 8
TILE = 256
OFFSETS = [o for o in (i * 37 % 128 for i in range(1, 128))]
PERMS = 8
QKVS = 4
ORDER = (2, 6, 4, 3, 7, 5, 1)
STEPS = 2
GROUP = 8
CHUNK = 256
HIDDEN = 768
MLPS = 4
EXP2_SCALE = 1.4426950408889634 * HEAD_DIM ** -0.5


def layer_norm(xf, gain, shift):
    mean = jnp.mean(xf, axis=-1, keepdims=True)
    cen = xf - mean
    var = jnp.mean(cen * cen, axis=-1, keepdims=True)
    return (cen * lax.rsqrt(var + LN_EPS) * gain + shift).astype(BF)


def dot(a, b):
    return jnp.dot(a, b, preferred_element_type=F32)


def dot_t(a, b):
    return lax.dot_general(a, b, (((1,), (1,)), ((), ())), preferred_element_type=F32)


def gelu(x):
    inner = x * (0.7978845608028654 + 0.035677408136300125 * (x * x))
    half = 0.5 * x
    return half + half * jnp.tanh(inner)


def score(q, k_at, keys, head, s_ref, m_ref):
    lane = lax.broadcasted_iota(jnp.int32, (TILE, 128), 1)
    qm = jnp.where(lax.div(lane, HEAD_DIM) == head % 2, q, jnp.zeros_like(q))
    slot = head % 2
    top = None
    step = keys // STEPS
    for c in range(STEPS):
        s = dot_t(k_at(c), qm)
        s_ref[slot, c * step:(c + 1) * step, :] = s
        t = jnp.max(s.reshape(step // GROUP, GROUP, TILE), axis=0)
        top = t if top is None else jnp.maximum(top, t)
        yield
    m_ref[slot] = jnp.broadcast_to(jnp.max(top, axis=0, keepdims=True), (8, TILE))
    yield


def mix(v_at, keys, head, s_ref, m_ref, out):
    slot = head % 2
    top = m_ref[slot, 0:1, :]
    total = None
    o = None
    step = keys // STEPS
    for c in range(STEPS):
        e = jnp.exp2((s_ref[slot, c * step:(c + 1) * step, :] - top) * EXP2_SCALE)
        t = jnp.sum(e.reshape(step // GROUP, GROUP, TILE), axis=0)
        total = t if total is None else total + t
        d = dot(v_at(c), e.astype(BF))
        o = d if o is None else o + d
        yield
    out.append(o * (1.0 / jnp.sum(total, axis=0, keepdims=True)))
    yield


def together(*steps):
    live = list(steps)
    while live:
        live = [g for g in live if next(g, live) is not live]


def attention(tiles, q_at, k_at, v_at, keys, s_ref, m_ref, put):
    def scores(t, head):
        return score(q_at(t, head // 2), lambda c: k_at(t, head // 2, c), keys, head, s_ref, m_ref)

    together(scores(0, 0))

    def step(t, carry):
        after = lax.rem(t + 1, tiles)
        out = []
        for head in range(HEADS):
            ahead = scores(t, head + 1) if head + 1 < HEADS else scores(after, 0)
            together(ahead, mix(lambda c: v_at(t, head, c), keys, head, s_ref, m_ref, out))
            if head % 2:
                put(t, head // 2, jnp.concatenate(out, axis=0).T.astype(BF))
                out = []
        return carry
    lax.fori_loop(0, tiles, step, 0)


def finish(xb, o, gain, shift, wout, wup, wdown, out):
    h = (xb.astype(F32) + dot(o, wout[...])).astype(BF)
    hf = h.astype(F32)
    yield
    a = layer_norm(hf, gain, shift)
    yield
    y = hf
    hidden = wup.shape[1]
    for c in range(0, hidden, HIDDEN):
        u = gelu(dot(a, wup[:, c:c + HIDDEN])).astype(BF)
        y = y + dot(u, wdown[c:c + HIDDEN, :])
        yield
    out.append(y)
    yield


def project(xb, gain, shift, wqk, wvt, put):
    a = layer_norm(xb.astype(F32), gain, shift)
    yield
    qk = dot(a, wqk[...]).astype(BF)
    yield
    put(qk, dot_t(wvt[...], a).astype(BF))
    yield


def kernel(ndev, frames, x_ref, gain_ref, shift_ref, wqkv_ref, wout_ref, wup_ref, wdown_ref, out_ref,
           wqk, qs, ks, vts, os_, sendbuf, recv, xt, q1, k1, v1t, o1, y1, s_scr, m_scr, send_sem, recv_sem, loc_sem):
    patches = ndev * SUBL
    width = HEADS * HEAD_DIM
    seq = frames * ndev
    me = lax.axis_index('sp')
    core, cx = lax.rem(me, 2), lax.rem(lax.div(me, 2), 4)
    cy, cz = lax.rem(lax.div(me, 8), 4), lax.div(me, 32)
    at_z = [lax.rem(cz + d, 4) * 32 for d in range(4)]
    at_y = [lax.rem(cy + d, 4) * 8 for d in range(4)]
    at_x = [lax.rem(cx + d, 4) * 2 for d in range(4)]
    at_core = [lax.rem(core + d, 2) for d in range(2)]
    nchunk = patches // CHUNK

    for l in range(2):
        wqk[l] = wqkv_ref[l, :2 * width, :].astype(F32).T.astype(BF)

    def send_to(stage, dst, j, to):
        pltpu.make_async_remote_copy(
            src_ref=sendbuf.at[stage, j, to], dst_ref=dst.at[j, me],
            send_sem=send_sem.at[stage, j], recv_sem=recv_sem.at[stage, j],
            device_id={'sp': to}, device_id_type=pl.DeviceIdType.MESH).start()

    def send_round(stage, dst, j):
        pltpu.make_async_copy(sendbuf.at[stage, j, me], dst.at[j, me], loc_sem.at[stage, j]).start()
        for d in OFFSETS:
            send_to(stage, dst, j, at_z[d // 32] + at_y[d // 8 % 4] + at_x[d // 2 % 4] + at_core[d % 2])

    def wait_bytes(ref, sem):
        pltpu.make_async_copy(ref, ref, sem).wait()

    def wait_arrived(stage, dst, j):
        pltpu.make_async_copy(sendbuf.at[stage, j, 0], dst.at[j, 0], loc_sem.at[stage, j]).wait()
        wait_bytes(dst.at[j, pl.ds(0, ndev - 1)], recv_sem.at[stage, j])

    def wait_sent(stage, j):
        wait_bytes(sendbuf.at[stage, j, pl.ds(0, ndev - 1)], send_sem.at[stage, j])

    def params(l):
        g = gain_ref[...].astype(F32)
        b = shift_ref[...].astype(F32)
        return g[2 * l:2 * l + 1], b[2 * l:2 * l + 1], g[2 * l + 1:2 * l + 2], b[2 * l + 1:2 * l + 2]

    ga, ba, gm, bm = params(0)

    def frame_step(j, carry):
        def qkv_step(c, cc):
            def put_at(rows):
                def put(qk, vt):
                    qs[rows, :] = qk[:, :width]
                    ks[rows, :] = qk[:, width:]
                    vts[:, rows] = vt
                return put
            rows = [pl.ds(pl.multiple_of((c * QKVS + i) * CHUNK, CHUNK), CHUNK) for i in range(QKVS)]
            together(*[project(x_ref[j, r, :], ga, ba, wqk.at[0], wqkv_ref.at[0, 2 * width:, :], put_at(r)) for r in rows])
            return cc
        lax.fori_loop(0, nchunk // QKVS, qkv_step, 0)

        def put(t, pair, o):
            os_[pl.ds(pl.multiple_of(t * TILE, TILE), TILE), 128 * pair:128 * pair + 128] = o
        attention(
            patches // TILE,
            lambda t, p: qs[pl.ds(pl.multiple_of(t * TILE, TILE), TILE), 128 * p:128 * p + 128],
            lambda t, p, c: ks[c * (patches // STEPS):(c + 1) * (patches // STEPS), 128 * p:128 * p + 128],
            lambda t, h, c: vts[HEAD_DIM * h:HEAD_DIM * h + HEAD_DIM, c * (patches // STEPS):(c + 1) * (patches // STEPS)],
            patches, s_scr, m_scr, put)

        def mlp_step(c, cc):
            outs = [[] for _ in range(MLPS)]
            rows = [pl.ds(pl.multiple_of((c * MLPS + i) * CHUNK, CHUNK), CHUNK) for i in range(MLPS)]
            together(*[finish(x_ref[j, r, :], os_[r, :], gm, bm, wout_ref.at[0], wup_ref.at[0], wdown_ref.at[0], out)
                       for r, out in zip(rows, outs)])
            dests = CHUNK // SUBL
            for i in range(MLPS):
                to = pl.ds(pl.multiple_of((c * MLPS + i) * dests, dests), dests)
                sendbuf[0, j, to] = outs[i][0].reshape(dests, SUBL, width).astype(BF)
            return cc
        lax.fori_loop(0, nchunk // MLPS, mlp_step, 0)
        send_round(0, recv, j)
        return carry

    lax.fori_loop(0, frames, frame_step, 0)

    ga, ba, gm, bm = params(1)
    r_io = lax.broadcasted_iota(jnp.int32, (128, 128), 0)
    c_io = lax.broadcasted_iota(jnp.int32, (128, 128), 1)
    to_seq = jnp.where((r_io // 16 == c_io % 8) & (r_io % 16 == c_io // 8), 1.0, 0.0).astype(BF)
    to_tok = jnp.where((r_io % 8 == c_io // 16) & (r_io // 8 == c_io % 16), 1.0, 0.0).astype(BF)

    def kv_step(j, carry):
        wait_arrived(0, recv, j)

        def perm_step(i, cc):
            for k in range(PERMS):
                g = i * PERMS + k
                blk = recv[j, pl.ds(g * 16, 16)].astype(F32).reshape(128, width).astype(BF)
                seqd = dot(to_seq, blk).astype(BF)
                for p in range(SUBL):
                    xt[j, p, pl.ds(pl.multiple_of(g * 16, 16), 16), :] = seqd[16 * p:16 * p + 16]
            return cc
        lax.fori_loop(0, ndev // 16 // PERMS, perm_step, 0)

        def qkv_step(c, cc):
            cols = pl.ds(pl.multiple_of(j * ndev, ndev), ndev)

            def put_at(first):
                def put(qk, vt):
                    for i in range(2):
                        part = slice(i * ndev, (i + 1) * ndev)
                        q1[first + i, cols, :] = qk[part, :width]
                        k1[first + i, cols, :] = qk[part, width:]
                        v1t[first + i, :, cols] = vt[:, part]
                return put
            firsts = [(c * QKVS + i) * 2 for i in range(QKVS)]
            together(*[project(xt[j, pl.ds(f, 2)].reshape(2 * ndev, width), ga, ba, wqk.at[1], wqkv_ref.at[1, 2 * width:, :], put_at(f))
                       for f in firsts])
            return cc
        lax.fori_loop(0, SUBL // 2 // QKVS, qkv_step, 0)
        return carry
    lax.fori_loop(0, frames, kv_step, 0)

    def time_step(jj, carry):
        first = pl.multiple_of(jj * TILE, TILE)

        def put(p, pair, o):
            o1[p, :, 128 * pair:128 * pair + 128] = o
        attention(
            SUBL,
            lambda t, p: q1[t, pl.ds(first, TILE), 128 * p:128 * p + 128],
            lambda t, p, c: k1[t, c * (seq // STEPS):(c + 1) * (seq // STEPS), 128 * p:128 * p + 128],
            lambda t, h, c: v1t[t, HEAD_DIM * h:HEAD_DIM * h + HEAD_DIM, c * (seq // STEPS):(c + 1) * (seq // STEPS)],
            seq, s_scr, m_scr, put)

        def half_step(half, carry):
            j = jj * (TILE // ndev) + half
            part = pl.ds(pl.multiple_of(half * ndev, ndev), ndev)

            def mlp_step(c, cc):
                outs = [[] for _ in range(MLPS)]
                at = [pl.ds((c * MLPS + i) * 2, 2) for i in range(MLPS)]
                together(*[finish(xt[j, r].reshape(CHUNK, width), o1[r, part, :].reshape(CHUNK, width), gm, bm,
                                  wout_ref.at[1], wup_ref.at[1], wdown_ref.at[1], out) for r, out in zip(at, outs)])
                for i in range(MLPS):
                    y1[at[i]] = outs[i][0].astype(BF).reshape(2, ndev, width)
                return cc
            lax.fori_loop(0, SUBL // 2 // MLPS, mlp_step, 0)

            def perm_step(i, cc):
                for k in range(PERMS):
                    g = i * PERMS + k
                    blk = y1[:, pl.ds(pl.multiple_of(g * 16, 16), 16), :].reshape(128, width)
                    tok = dot(to_tok, blk)
                    sendbuf[1, j, pl.ds(g * 16, 16)] = tok.reshape(16, SUBL, width).astype(BF)
                return cc
            lax.fori_loop(0, ndev // 16 // PERMS, perm_step, 0)
            send_round(1, out_ref, j)
            return carry
        lax.fori_loop(0, TILE // ndev, half_step, 0)
        return carry

    lax.fori_loop(0, seq // TILE, time_step, 0)

    def drain(j, carry):
        wait_sent(0, j)
        wait_sent(1, j)
        wait_arrived(1, out_ref, j)
        return carry
    lax.fori_loop(0, frames, drain, 0)


def solution(mesh):
    ndev = mesh.shape['sp']
    act_spec = P('data', 'sp', None, None)

    def local_run(latent, ln_gain, ln_bias, w_qkv, w_out, w_up, w_down):
        _, frames, patches, width = latent.shape
        wqkv_t = w_qkv.transpose(0, 2, 3, 4, 1).reshape(2, 3 * width, width)
        seq = frames * ndev
        out = pl.pallas_call(
            functools.partial(kernel, ndev, frames),
            out_shape=jax.ShapeDtypeStruct((frames, ndev, SUBL, width), BF),
            in_specs=[pl.BlockSpec(memory_space=pltpu.VMEM)] * 7,
            out_specs=pl.BlockSpec(memory_space=pl.ANY),
            scratch_shapes=[
                pltpu.VMEM((2, width, 2 * width), BF),
                pltpu.VMEM((patches, width), BF),
                pltpu.VMEM((patches, width), BF),
                pltpu.VMEM((width, patches), BF),
                pltpu.VMEM((patches, width), BF),
                pltpu.VMEM((2, frames, ndev, SUBL, width), BF),
                pltpu.VMEM((frames, ndev, SUBL, width), BF),
                pltpu.VMEM((frames, SUBL, ndev, width), BF),
                pltpu.VMEM((SUBL, seq, width), BF),
                pltpu.VMEM((SUBL, seq, width), BF),
                pltpu.VMEM((SUBL, width, seq), BF),
                pltpu.VMEM((SUBL, 2 * ndev, width), BF),
                pltpu.VMEM((SUBL, ndev, width), BF),
                pltpu.VMEM((2, max(patches, seq), TILE), F32),
                pltpu.VMEM((2, 8, TILE), F32),
                pltpu.SemaphoreType.DMA((2, frames)),
                pltpu.SemaphoreType.DMA((2, frames)),
                pltpu.SemaphoreType.DMA((2, frames)),
            ],
            compiler_params=pltpu.CompilerParams(has_side_effects=True, vmem_limit_bytes=67043328),
            name='latte_blocks',
        )(latent[0], ln_gain, ln_bias, wqkv_t, w_out.reshape(2, width, width), w_up, w_down)
        return out.reshape(1, frames, patches, width)

    return jax.shard_map(local_run, mesh=mesh, in_specs=(act_spec, P(), P(), P(), P(), P(), P()), out_specs=act_spec, check_vma=False)
```

```python
import functools
import jax
import jax.numpy as jnp
from jax import lax
from jax.experimental import pallas as pl
from jax.experimental.pallas import tpu as pltpu
from jax.sharding import PartitionSpec as P

LN_EPS = 1e-6
HEADS = 6
HEAD_DIM = 64
BF = jnp.bfloat16
F32 = jnp.float32
SUBL = 8
TILE = 256
OFFSETS = [o for o in (i * 37 % 128 for i in range(1, 128))]
PERMS = 8
TILES = 4
QKVS = 4
ORDER = (2, 6, 4, 3, 7, 5, 1)
STEPS = 2
GROUP = 8
CHUNK = 256
HIDDEN = 768
MLPS = 4
EXP2_SCALE = 1.4426950408889634 * HEAD_DIM ** -0.5


def layer_norm(xf, gain, shift):
    mean = jnp.mean(xf, axis=-1, keepdims=True)
    cen = xf - mean
    var = jnp.mean(cen * cen, axis=-1, keepdims=True)
    return (cen * lax.rsqrt(var + LN_EPS) * gain + shift).astype(BF)


def dot(a, b):
    return jnp.dot(a, b, preferred_element_type=F32)


def dot_t(a, b):
    return lax.dot_general(a, b, (((1,), (1,)), ((), ())), preferred_element_type=F32)


def gelu(x):
    inner = x * (0.7978845608028654 + 0.035677408136300125 * (x * x))
    half = 0.5 * x
    return half + half * jnp.tanh(inner)


def score(q, k_at, keys, head, s_ref, m_ref):
    lane = lax.broadcasted_iota(jnp.int32, (TILE, 128), 1)
    qm = jnp.where(lax.div(lane, HEAD_DIM) == head % 2, q, jnp.zeros_like(q))
    slot = head
    top = None
    step = keys // STEPS
    for c in range(STEPS):
        s = dot_t(k_at(c), qm)
        s_ref[slot, c * step:(c + 1) * step, :] = s
        t = jnp.max(s.reshape(step // GROUP, GROUP, TILE), axis=0)
        top = t if top is None else jnp.maximum(top, t)
        yield
    m_ref[slot] = jnp.broadcast_to(jnp.max(top, axis=0, keepdims=True), (8, TILE))
    yield


def mix(v_at, keys, head, s_ref, m_ref, out):
    slot = head
    top = m_ref[slot, 0:1, :]
    total = None
    o = None
    step = keys // STEPS
    for c in range(STEPS):
        e = jnp.exp2((s_ref[slot, c * step:(c + 1) * step, :] - top) * EXP2_SCALE)
        t = jnp.sum(e.reshape(step // GROUP, GROUP, TILE), axis=0)
        total = t if total is None else total + t
        d = dot(v_at(c), e.astype(BF))
        o = d if o is None else o + d
        yield
    out.append(o * (1.0 / jnp.sum(total, axis=0, keepdims=True)))
    yield


def together(*steps):
    live = list(steps)
    while live:
        live = [g for g in live if next(g, live) is not live]


def attention(tiles, q_at, k_at, v_at, keys, s_ref, m_ref, put):
    def scores(t, head):
        return score(q_at(t, head // 2), lambda c: k_at(t, head // 2, c), keys, head, s_ref, m_ref)

    together(scores(0, 0), scores(0, 1))

    def tile(t, after):
        for head in range(0, HEADS, 2):
            heads = (head, head + 1)
            ahead = [scores(t, h + 2) if head + 2 < HEADS else scores(after, h + 2 - HEADS) for h in heads]
            outs = [[], []]
            together(*ahead, *[mix(lambda c, h=h: v_at(t, h, c), keys, h, s_ref, m_ref, out) for h, out in zip(heads, outs)])
            put(t, head // 2, jnp.concatenate([out[0] for out in outs], axis=0).T.astype(BF))

    def step(i, carry):
        for k in range(TILES):
            t = i * TILES + k
            tile(t, t + 1 if k + 1 < TILES else lax.rem(t + 1, tiles))
        return carry
    lax.fori_loop(0, tiles // TILES, step, 0)


def finish(xb, o, gain, shift, wout, wup, wdown, out):
    h = (xb.astype(F32) + dot(o, wout[...])).astype(BF)
    hf = h.astype(F32)
    yield
    a = layer_norm(hf, gain, shift)
    yield
    y = hf
    hidden = wup.shape[1]
    for c in range(0, hidden, HIDDEN):
        u = gelu(dot(a, wup[:, c:c + HIDDEN])).astype(BF)
        y = y + dot(u, wdown[c:c + HIDDEN, :])
        yield
    out.append(y)
    yield


def project(xb, gain, shift, wqk, wvt, put):
    a = layer_norm(xb.astype(F32), gain, shift)
    yield
    qk = dot(a, wqk[...]).astype(BF)
    yield
    put(qk, dot_t(wvt[...], a).astype(BF))
    yield


def kernel(ndev, frames, x_hbm, gain_ref, shift_ref, wqkv_hbm, wout_hbm, wup_hbm, wdown_hbm, out_ref,
           x_ref, wqkv_ref, wout_ref, wup_ref, wdown_ref, x_sem, w_sem,
           wqk, qs, ks, vts, os_, sendbuf, recv, xt, q1, k1, v1t, o1, y1, s_scr, m_scr, send_sem, recv_sem, loc_sem):
    patches = ndev * SUBL
    width = HEADS * HEAD_DIM
    seq = frames * ndev
    me = lax.axis_index('sp')
    core, cx = lax.rem(me, 2), lax.rem(lax.div(me, 2), 4)
    cy, cz = lax.rem(lax.div(me, 8), 4), lax.div(me, 32)
    at_z = [lax.rem(cz + d, 4) * 32 for d in range(4)]
    at_y = [lax.rem(cy + d, 4) * 8 for d in range(4)]
    at_x = [lax.rem(cx + d, 4) * 2 for d in range(4)]
    at_core = [lax.rem(core + d, 2) for d in range(2)]
    nchunk = patches // CHUNK

    weights = ((wqkv_hbm, wqkv_ref), (wout_hbm, wout_ref), (wup_hbm, wup_ref), (wdown_hbm, wdown_ref))

    def load_frame(j):
        return pltpu.make_async_copy(x_hbm.at[j], x_ref.at[j], x_sem.at[j])

    def load_weights(l):
        return [pltpu.make_async_copy(src.at[l], dst.at[l], w_sem.at[l, i]) for i, (src, dst) in enumerate(weights)]

    def start_weights(l):
        for copy in load_weights(l):
            copy.start()

    def wait_weights(l):
        for copy in load_weights(l):
            copy.wait()
        wqk[l] = wqkv_ref[l, :2 * width, :].astype(F32).T.astype(BF)

    start_weights(0)
    for j in range(frames):
        load_frame(j).start()
    start_weights(1)
    wait_weights(0)

    def send_to(stage, dst, j, to):
        pltpu.make_async_remote_copy(
            src_ref=sendbuf.at[stage, j, to], dst_ref=dst.at[j, me],
            send_sem=send_sem.at[stage, j], recv_sem=recv_sem.at[stage, j],
            device_id={'sp': to}, device_id_type=pl.DeviceIdType.MESH).start()

    def send_round(stage, dst, j):
        pltpu.make_async_copy(sendbuf.at[stage, j, me], dst.at[j, me], loc_sem.at[stage, j]).start()
        for d in OFFSETS:
            send_to(stage, dst, j, at_z[d // 32] + at_y[d // 8 % 4] + at_x[d // 2 % 4] + at_core[d % 2])

    def wait_bytes(ref, sem):
        pltpu.make_async_copy(ref, ref, sem).wait()

    def wait_arrived(stage, dst, j):
        pltpu.make_async_copy(sendbuf.at[stage, j, 0], dst.at[j, 0], loc_sem.at[stage, j]).wait()
        wait_bytes(dst.at[j, pl.ds(0, ndev - 1)], recv_sem.at[stage, j])

    def wait_sent(stage, j):
        wait_bytes(sendbuf.at[stage, j, pl.ds(0, ndev - 1)], send_sem.at[stage, j])

    def params(l):
        g = gain_ref[...].astype(F32)
        b = shift_ref[...].astype(F32)
        return g[2 * l:2 * l + 1], b[2 * l:2 * l + 1], g[2 * l + 1:2 * l + 2], b[2 * l + 1:2 * l + 2]

    ga, ba, gm, bm = params(0)

    def frame_step(j, carry):
        load_frame(j).wait()

        def qkv_step(c, cc):
            def put_at(rows):
                def put(qk, vt):
                    qs[rows, :] = qk[:, :width]
                    ks[rows, :] = qk[:, width:]
                    vts[:, rows] = vt
                return put
            rows = [pl.ds(pl.multiple_of((c * QKVS + i) * CHUNK, CHUNK), CHUNK) for i in range(QKVS)]
            together(*[project(x_ref[j, r, :], ga, ba, wqk.at[0], wqkv_ref.at[0, 2 * width:, :], put_at(r)) for r in rows])
            return cc
        lax.fori_loop(0, nchunk // QKVS, qkv_step, 0)

        def put(t, pair, o):
            os_[pl.ds(pl.multiple_of(t * TILE, TILE), TILE), 128 * pair:128 * pair + 128] = o
        attention(
            patches // TILE,
            lambda t, p: qs[pl.ds(pl.multiple_of(t * TILE, TILE), TILE), 128 * p:128 * p + 128],
            lambda t, p, c: ks[c * (patches // STEPS):(c + 1) * (patches // STEPS), 128 * p:128 * p + 128],
            lambda t, h, c: vts[HEAD_DIM * h:HEAD_DIM * h + HEAD_DIM, c * (patches // STEPS):(c + 1) * (patches // STEPS)],
            patches, s_scr, m_scr, put)

        def mlp_step(c, cc):
            outs = [[] for _ in range(MLPS)]
            rows = [pl.ds(pl.multiple_of((c * MLPS + i) * CHUNK, CHUNK), CHUNK) for i in range(MLPS)]
            together(*[finish(x_ref[j, r, :], os_[r, :], gm, bm, wout_ref.at[0], wup_ref.at[0], wdown_ref.at[0], out)
                       for r, out in zip(rows, outs)])
            dests = CHUNK // SUBL
            for i in range(MLPS):
                to = pl.ds(pl.multiple_of((c * MLPS + i) * dests, dests), dests)
                sendbuf[0, j, to] = outs[i][0].reshape(dests, SUBL, width).astype(BF)
            return cc
        lax.fori_loop(0, nchunk // MLPS, mlp_step, 0)
        send_round(0, recv, j)
        return carry

    lax.fori_loop(0, frames, frame_step, 0)
    wait_weights(1)

    ga, ba, gm, bm = params(1)
    r_io = lax.broadcasted_iota(jnp.int32, (128, 128), 0)
    c_io = lax.broadcasted_iota(jnp.int32, (128, 128), 1)
    to_seq = jnp.where((r_io // 16 == c_io % 8) & (r_io % 16 == c_io // 8), 1.0, 0.0).astype(BF)
    to_tok = jnp.where((r_io % 8 == c_io // 16) & (r_io // 8 == c_io % 16), 1.0, 0.0).astype(BF)

    def kv_step(j, carry):
        wait_arrived(0, recv, j)

        def perm_step(i, cc):
            for k in range(PERMS):
                g = i * PERMS + k
                blk = recv[j, pl.ds(g * 16, 16)].astype(F32).reshape(128, width).astype(BF)
                seqd = dot(to_seq, blk).astype(BF)
                for p in range(SUBL):
                    xt[j, p, pl.ds(pl.multiple_of(g * 16, 16), 16), :] = seqd[16 * p:16 * p + 16]
            return cc
        lax.fori_loop(0, ndev // 16 // PERMS, perm_step, 0)

        def qkv_step(c, cc):
            cols = pl.ds(pl.multiple_of(j * ndev, ndev), ndev)

            def put_at(first):
                def put(qk, vt):
                    for i in range(2):
                        part = slice(i * ndev, (i + 1) * ndev)
                        q1[first + i, cols, :] = qk[part, :width]
                        k1[first + i, cols, :] = qk[part, width:]
                        v1t[first + i, :, cols] = vt[:, part]
                return put
            firsts = [(c * QKVS + i) * 2 for i in range(QKVS)]
            together(*[project(xt[j, pl.ds(f, 2)].reshape(2 * ndev, width), ga, ba, wqk.at[1], wqkv_ref.at[1, 2 * width:, :], put_at(f))
                       for f in firsts])
            return cc
        lax.fori_loop(0, SUBL // 2 // QKVS, qkv_step, 0)
        return carry
    lax.fori_loop(0, frames, kv_step, 0)

    def time_step(jj, carry):
        first = pl.multiple_of(jj * TILE, TILE)

        def put(p, pair, o):
            o1[p, :, 128 * pair:128 * pair + 128] = o
        attention(
            SUBL,
            lambda t, p: q1[t, pl.ds(first, TILE), 128 * p:128 * p + 128],
            lambda t, p, c: k1[t, c * (seq // STEPS):(c + 1) * (seq // STEPS), 128 * p:128 * p + 128],
            lambda t, h, c: v1t[t, HEAD_DIM * h:HEAD_DIM * h + HEAD_DIM, c * (seq // STEPS):(c + 1) * (seq // STEPS)],
            seq, s_scr, m_scr, put)

        def half_step(half, carry):
            j = jj * (TILE // ndev) + half
            part = pl.ds(pl.multiple_of(half * ndev, ndev), ndev)

            def mlp_step(c, cc):
                outs = [[] for _ in range(MLPS)]
                at = [pl.ds((c * MLPS + i) * 2, 2) for i in range(MLPS)]
                together(*[finish(xt[j, r].reshape(CHUNK, width), o1[r, part, :].reshape(CHUNK, width), gm, bm,
                                  wout_ref.at[1], wup_ref.at[1], wdown_ref.at[1], out) for r, out in zip(at, outs)])
                for i in range(MLPS):
                    y1[at[i]] = outs[i][0].astype(BF).reshape(2, ndev, width)
                return cc
            lax.fori_loop(0, SUBL // 2 // MLPS, mlp_step, 0)

            def perm_step(i, cc):
                for k in range(PERMS):
                    g = i * PERMS + k
                    blk = y1[:, pl.ds(pl.multiple_of(g * 16, 16), 16), :].reshape(128, width)
                    tok = dot(to_tok, blk)
                    sendbuf[1, j, pl.ds(g * 16, 16)] = tok.reshape(16, SUBL, width).astype(BF)
                return cc
            lax.fori_loop(0, ndev // 16 // PERMS, perm_step, 0)
            send_round(1, out_ref, j)
            return carry
        lax.fori_loop(0, TILE // ndev, half_step, 0)
        return carry

    lax.fori_loop(0, seq // TILE, time_step, 0)

    def drain(j, carry):
        wait_sent(0, j)
        wait_sent(1, j)
        wait_arrived(1, out_ref, j)
        return carry
    lax.fori_loop(0, frames, drain, 0)


def solution(mesh):
    ndev = mesh.shape['sp']
    act_spec = P('data', 'sp', None, None)

    def local_run(latent, ln_gain, ln_bias, w_qkv, w_out, w_up, w_down):
        _, frames, patches, width = latent.shape
        wqkv_t = w_qkv.transpose(0, 2, 3, 4, 1).reshape(2, 3 * width, width)
        seq = frames * ndev
        any_spec, vmem_spec = pl.BlockSpec(memory_space=pl.ANY), pl.BlockSpec(memory_space=pltpu.VMEM)
        hidden = w_up.shape[2]
        out = pl.pallas_call(
            functools.partial(kernel, ndev, frames),
            out_shape=jax.ShapeDtypeStruct((frames, ndev, SUBL, width), BF),
            in_specs=[any_spec, vmem_spec, vmem_spec] + [any_spec] * 4,
            out_specs=pl.BlockSpec(memory_space=pl.ANY),
            scratch_shapes=[
                pltpu.VMEM((frames, patches, width), BF),
                pltpu.VMEM((2, 3 * width, width), BF),
                pltpu.VMEM((2, width, width), BF),
                pltpu.VMEM((2, width, hidden), BF),
                pltpu.VMEM((2, hidden, width), BF),
                pltpu.SemaphoreType.DMA((frames,)),
                pltpu.SemaphoreType.DMA((2, 4)),
                pltpu.VMEM((2, width, 2 * width), BF),
                pltpu.VMEM((patches, width), BF),
                pltpu.VMEM((patches, width), BF),
                pltpu.VMEM((width, patches), BF),
                pltpu.VMEM((patches, width), BF),
                pltpu.VMEM((2, frames, ndev, SUBL, width), BF),
                pltpu.VMEM((frames, ndev, SUBL, width), BF),
                pltpu.VMEM((frames, SUBL, ndev, width), BF),
                pltpu.VMEM((SUBL, seq, width), BF),
                pltpu.VMEM((SUBL, seq, width), BF),
                pltpu.VMEM((SUBL, width, seq), BF),
                pltpu.VMEM((SUBL, 2 * ndev, width), BF),
                pltpu.VMEM((SUBL, ndev, width), BF),
                pltpu.VMEM((HEADS, max(patches, seq), TILE), F32),
                pltpu.VMEM((HEADS, 8, TILE), F32),
                pltpu.SemaphoreType.DMA((2, frames)),
                pltpu.SemaphoreType.DMA((2, frames)),
                pltpu.SemaphoreType.DMA((2, frames)),
            ],
            compiler_params=pltpu.CompilerParams(has_side_effects=True, vmem_limit_bytes=67043328),
            name='latte_blocks',
        )(latent[0], ln_gain, ln_bias, wqkv_t, w_out.reshape(2, width, width), w_up, w_down)
        return out.reshape(1, frames, patches, width)

    return jax.shard_map(local_run, mesh=mesh, in_specs=(act_spec, P(), P(), P(), P(), P(), P()), out_specs=act_spec, check_vma=False)
```
